32 devices in a mesh: mission: 2 (over x), arc: 16 (over z, y, core).
Axes of the slice: x: 2, y: 2, z: 4, core: 2. Of those that a mesh axis runs over, the one named last changes fastest.
Arguments:
- design: bfloat16 [2560, 5120], P(('mission', 'arc')), may hold values from -3 to 3
- nuisance_design: bfloat16 [2560, 128], P(('mission', 'arc')), may hold values from -1 to 1
- observed: float32 [2560], P(('mission', 'arc')), may hold values from -6 to 6
- arc_of_row: int32 [2560], P(('mission', 'arc')), may hold values from 0 to 1, as said below
- nuis_size: int32 [64], P(('mission', 'arc')), may hold values from 32 to 128
- weight_index: int32 [2560], P(('mission', 'arc')), may hold values from 0 to 7
- kind_weight: float32 [8], replicated, may hold values from 0.3 to 3
- mission_weight: float32 [2], P('mission'), may hold values from 0.3 to 3
Outputs:
- normal_fold: float32 [2560, 5120], P(('mission', 'arc'))
- right_side: float32 [5120], P(('mission', 'arc'))
- tail_diagonal: float32 [2560], P(('mission', 'arc'))
The draws below stay inside these ranges and needn't reach their ends.
Inputs may be any that keep to these rules, and one draw needn't show every extreme that they name: `arc_of_row`: in each row block of 80 rows the rows of arc 0 come first and those of arc 1 follow; each arc has at least 20 rows.
All inputs are finite; a program needn't handle non-finite values.
Results may differ from the reference program's by a relative error of at most 0.019.
Values may be sent and summed in bfloat16 or wider, within the bound.
A program may use at most 192 MiB of HBM per device.

```python
import math
import jax
import jax.numpy as jnp
from jax import lax

P_SIZE = 5120
NUIS = 128
KINDS = 8
ARCS_DEV = 2
OBS_DEV = 80
HALF = 2560
OBS = 2560
ARCS = 64
N_MISSION = 2
N_ARC = 16


def draw_design(key, part):
    noise_key = jax.random.fold_in(jax.random.fold_in(key, 11), 0)
    freq_key = jax.random.fold_in(jax.random.fold_in(key, 11), 1)
    phase_key = jax.random.fold_in(jax.random.fold_in(key, 11), 2)
    perm_key = jax.random.fold_in(jax.random.fold_in(key, 11), 4)
    columns = jnp.arange(P_SIZE, dtype=jnp.float32)
    noise_part = jnp.clip(jax.random.normal(noise_key, (OBS, P_SIZE), jnp.float32), -6.0, 6.0)
    mode_count = 4
    frequency = jnp.exp(jax.random.uniform(freq_key, (OBS, mode_count), jnp.float32, math.log(0.001), 0.0))
    phases = jax.random.uniform(phase_key, (OBS, mode_count), jnp.float32, -math.pi, math.pi)
    smooth = jnp.zeros((OBS, P_SIZE), jnp.float32)
    for mode_id in range(mode_count):
        smooth = smooth + jnp.cos(frequency[:, mode_id:mode_id + 1] * columns[None, :] + phases[:, mode_id:mode_id + 1])
    values = noise_part + math.sqrt(2.0 / mode_count) * smooth
    blocks = OBS // OBS_DEV
    block_width = P_SIZE // blocks
    target = jax.random.permutation(perm_key, blocks)
    row_block = jnp.arange(OBS, dtype=jnp.int32) // OBS_DEV
    col_block = jnp.arange(P_SIZE, dtype=jnp.int32) // block_width
    spike_gain = jnp.where(target[row_block][:, None] == col_block[None, :], 6.0, 1.0)
    scaled = values * spike_gain / math.sqrt(OBS)
    return jnp.clip(scaled, -3.0, 3.0).astype(jnp.bfloat16)


def draw_arc_of_row(key, part):
    blocks = OBS // OBS_DEV
    split_at = jax.random.randint(jax.random.fold_in(key, 23), (blocks, 1), OBS_DEV // 4, 3 * OBS_DEV // 4 + 1)
    position = jnp.arange(OBS_DEV, dtype=jnp.int32)[None, :]
    return (position >= split_at).astype(jnp.int32).reshape(OBS)


def touch_ends(values, rng, least, top_value):
    shape = values.shape
    index_at = [jax.random.randint(jax.random.fold_in(rng, axis), (), 0, shape[axis]) for axis in range(len(shape))]
    values = values.at[tuple(index_at)].set(least)
    longest = shape.index(max(shape))
    index_at[longest] = (index_at[longest] + 1) % shape[longest]
    return values.at[tuple(index_at)].set(top_value)


def block_levels(key, extent, pieces, least, top_value):
    loudness = 1.0
    for axis_at, parts in pieces:
        steps = jax.random.uniform(jax.random.fold_in(jax.random.fold_in(key, 6), axis_at), (parts,), jnp.float32, least / len(pieces), top_value / len(pieces))
        loudness = loudness * jnp.repeat(jnp.exp(steps), extent[axis_at] // parts).reshape((-1,) + (1,) * (len(extent) - 1 - axis_at))
    return loudness


def normal_values(key, dims, deviation, reach, cuts=(), held_as=jnp.bfloat16):
    level = block_levels(key, dims, cuts, -0.22, 0.18) if cuts else 1.0
    array = jax.random.normal(key, dims, jnp.float32) * deviation * level
    return jnp.minimum(jnp.maximum(array, -reach), reach).astype(held_as)


def setup_inputs(seed: int = 0) -> dict:
    keys = jax.random.split(jax.random.key(seed), 9)
    return {
        "design": draw_design(jax.random.fold_in(keys[8], 71), 0),
        "nuisance_design": normal_values(keys[1], (OBS, NUIS), (OBS_DEV // 2) ** -0.5, 1.0, ((0, 32),)),
        "observed": normal_values(keys[2], (OBS,), 1.0, 6.0, ((0, 32),), jnp.float32),
        "arc_of_row": draw_arc_of_row(jax.random.fold_in(keys[8], 71), 0),
        "nuis_size": touch_ends(jax.random.randint(keys[4], (ARCS,), NUIS // 4, NUIS + 1), jax.random.fold_in(keys[4], 1), NUIS // 4, NUIS).astype(jnp.int32),
        "weight_index": touch_ends(jax.random.randint(keys[5], (OBS,), 0, KINDS), jax.random.fold_in(keys[5], 1), 0, KINDS - 1).astype(jnp.int32),
        "kind_weight": jnp.clip(jnp.exp(jax.random.uniform(keys[6], (KINDS,), jnp.float32, math.log(0.3), math.log(3.0))), 0.3, 3.0),
        "mission_weight": jnp.clip(jnp.exp(math.log(3.0) - 2.3025851 * jax.random.uniform(keys[7], (N_MISSION,), jnp.float32) ** block_levels(keys[7], (N_MISSION,), ((0, 2),), -0.2, 0.2)), 0.3, 3.0),
    }


def local_system(design, nuisance_design, observed, arc_of_row, nuis_size, weight_index, kind_weight):
    kind_ids = jnp.arange(kind_weight.shape[0], dtype=jnp.int32)
    row_weight = jnp.sum(jnp.where(weight_index[:, None] == kind_ids[None, :], kind_weight[None, :], 0.0), axis=1)
    nuis_ids = jnp.arange(nuisance_design.shape[1], dtype=jnp.int32)
    eye_block = jnp.eye(nuisance_design.shape[1], dtype=jnp.float32)
    blocks = []
    solved = []
    solved_obs = []
    for arc_id in range(ARCS_DEV):
        col_mask = (nuis_ids < nuis_size[arc_id]).astype(jnp.bfloat16)
        in_arc = (arc_of_row == arc_id).astype(jnp.float32)
        masked = nuisance_design * col_mask[None, :]
        weighted = (masked.astype(jnp.float32) * (row_weight * in_arc)[:, None]).astype(jnp.bfloat16)
        normal_ll = jnp.dot(weighted.T.astype(jnp.float32), masked.astype(jnp.float32), preferred_element_type=jnp.float32) + eye_block
        coupling = jnp.dot(weighted.T.astype(jnp.float32), design.astype(jnp.float32), preferred_element_type=jnp.float32)
        obs_part = jnp.dot(weighted.T.astype(jnp.float32), observed, precision=lax.Precision.HIGHEST)
        factor = jnp.linalg.cholesky(normal_ll)
        blocks.append(weighted)
        solved.append(jax.scipy.linalg.cho_solve((factor, True), coupling).astype(jnp.bfloat16))
        solved_obs.append(jax.scipy.linalg.cho_solve((factor, True), obs_part))
    stacked = jnp.concatenate(blocks, axis=1)
    solved_all = jnp.concatenate(solved, axis=0)
    obs_all = jnp.concatenate(solved_obs, axis=0)
    reduced = (row_weight[:, None] * design.astype(jnp.float32) - jnp.dot(stacked.astype(jnp.float32), solved_all.astype(jnp.float32), preferred_element_type=jnp.float32)).astype(jnp.bfloat16)
    reduced_obs = (row_weight * observed - jnp.dot(stacked.astype(jnp.float32), obs_all, precision=lax.Precision.HIGHEST)).astype(jnp.bfloat16)
    right_term = jnp.dot(reduced_obs.astype(jnp.float32), design.astype(jnp.float32), preferred_element_type=jnp.float32)
    half_width = design.shape[1] // 2
    tail_term = jnp.sum(design[:, half_width:].astype(jnp.float32) * reduced[:, half_width:].astype(jnp.float32), axis=0)
    return (reduced, right_term, tail_term)

def reference(design, nuisance_design, observed, arc_of_row, nuis_size, weight_index, kind_weight, mission_weight):
    devices = N_MISSION * N_ARC
    col_ids = jnp.arange(P_SIZE, dtype=jnp.int32)
    row_ids = jnp.arange(HALF, dtype=jnp.int32)
    keep_upper = col_ids[None, :] >= row_ids[:, None]

    def per_block(totals, block_id):
        fold_total, right_total, tail_total = totals
        row_start = (block_id * OBS_DEV).astype(jnp.int32)
        arc_start = (block_id * ARCS_DEV).astype(jnp.int32)
        block_design = lax.dynamic_slice_in_dim(design, row_start, OBS_DEV, 0)
        block_nuis = lax.dynamic_slice_in_dim(nuisance_design, row_start, OBS_DEV, 0)
        block_obs = lax.dynamic_slice_in_dim(observed, row_start, OBS_DEV, 0)
        block_arcs = lax.dynamic_slice_in_dim(arc_of_row, row_start, OBS_DEV, 0)
        block_kinds = lax.dynamic_slice_in_dim(weight_index, row_start, OBS_DEV, 0)
        block_sizes = lax.dynamic_slice_in_dim(nuis_size, arc_start, ARCS_DEV, 0)
        weight = mission_weight[block_id // N_ARC]
        reduced, right_term, tail_term = local_system(block_design, block_nuis, block_obs, block_arcs, block_sizes, block_kinds, kind_weight)
        term_full = weight * jnp.dot(block_design.T.astype(jnp.float32), reduced.astype(jnp.float32), preferred_element_type=jnp.float32)
        folded = jnp.where(keep_upper, term_full[:HALF], term_full[::-1, ::-1][:HALF])
        rounded = lax.optimization_barrier(folded.astype(jnp.bfloat16))
        fold_total = fold_total + rounded.astype(jnp.float32)
        return ((fold_total, right_total + weight * right_term, tail_total + weight * tail_term), None)
    initial = (jnp.zeros((HALF, P_SIZE), jnp.float32), jnp.zeros((P_SIZE,), jnp.float32), jnp.zeros((HALF,), jnp.float32))
    totals, unused_out = lax.scan(per_block, initial, jnp.arange(devices, dtype=jnp.int32))
    return (totals[0], totals[1], totals[2])
```

```python
import functools

import jax
import jax.numpy as jnp
import numpy as np
from jax import lax
from jax.experimental import pallas as pl
from jax.experimental.pallas import tpu as pltpu
from jax.sharding import PartitionSpec as P

LANES = 128


def rounded_up(value, unit):
    return -(-value // unit) * unit


def projector_kernel(
    sizes_ref, kinds_ref, nuis_ref, arc_col_ref, arc_row_ref, kind_col_ref, obs_row_ref, out_ref
):
    rows, wide = out_ref.shape
    arc_col = arc_col_ref[...]
    kind_col = kind_col_ref[...]
    weight = jnp.zeros((rows, 1), jnp.float32)
    for kind in range(kinds_ref.shape[0]):
        weight = jnp.where(kind_col == kind, kinds_ref[kind], weight)
    size = jnp.zeros((rows, 1), jnp.int32)
    for arc in range(sizes_ref.shape[0]):
        size = jnp.where(arc_col == arc, sizes_ref[arc], size)
    nuis = nuis_ref[...].astype(jnp.float32)
    nuis = jnp.where(lax.broadcasted_iota(jnp.int32, nuis.shape, 1) < size, nuis, 0.0)
    padded = jnp.concatenate(
        [nuis, jnp.zeros((wide - rows, nuis.shape[1]), jnp.float32)], axis=0
    )
    gram = lax.dot_general(
        nuis.astype(jnp.bfloat16),
        padded.astype(jnp.bfloat16),
        (((1,), (1,)), ((), ())),
        preferred_element_type=jnp.float32,
    )
    lane = lax.broadcasted_iota(jnp.int32, (rows, wide), 1)
    sub = lax.broadcasted_iota(jnp.int32, (rows, wide), 0)
    state = jnp.where(arc_col == arc_row_ref[...], gram, 0.0)
    state = state + jnp.where(lane == sub, 1.0 / weight, 0.0)
    for k in range(rows):
        row = state[k : k + 1, :]
        col = state[:, k : k + 1]
        inv = 1.0 / row[:, k : k + 1]
        scaled_row = row * inv
        scaled_col = col * inv
        swept = state - col * scaled_row
        swept = jnp.where(lane == k, scaled_col, swept)
        swept = jnp.where(sub == k, scaled_row, swept)
        state = jnp.where((lane == k) & (sub == k), -inv, swept)
    inverse = -state
    reduced_obs = jnp.sum(inverse * obs_row_ref[...], axis=1, keepdims=True)
    out_ref[...] = jnp.where(lane == rows, reduced_obs, inverse).astype(out_ref.dtype)


def fold_kernel(
    block_rows,
    width,
    weight_ref,
    proj_ref,
    picked_ref,
    perm_ref,
    rows_ref,
    above_ref,
    mirror_ref,
    fold_ref,
    right_ref,
    tail_ref,
    lhs_ref,
):
    tile = pl.program_id(0)
    tile_cols = above_ref.shape[1]
    out_rows = fold_ref.shape[0]
    weight = weight_ref[0]

    @pl.when(tile == 0)
    def _():
        tail = jnp.zeros((1, width), jnp.float32)
        lane = lax.broadcasted_iota(jnp.int32, (block_rows, width), 1)
        pieces = []
        for block in range(proj_ref.shape[0] // block_rows):
            span = pl.ds(block * block_rows, block_rows)
            proj = proj_ref[span, :]
            picked = picked_ref[span, :]
            reduced = lax.dot_general(
                proj[:, :block_rows], picked, (((1,), (0,)), ((), ())),
                preferred_element_type=jnp.float32,
            )
            tail_reduced = reduced[:, 2 * width :].astype(jnp.bfloat16).astype(jnp.float32)
            tail += jnp.sum(
                picked[:, 2 * width :].astype(jnp.float32) * tail_reduced, axis=0, keepdims=True
            )
            first = jnp.where(
                lane == width - 1,
                proj[:, block_rows : block_rows + 1].astype(jnp.float32),
                reduced[:, :width],
            )
            second = jnp.dot(
                reduced[:, width : 2 * width].astype(jnp.bfloat16),
                perm_ref[...],
                preferred_element_type=jnp.float32,
            )
            pieces.append(jnp.concatenate([first, second], axis=1))
        lhs_ref[...] = jnp.concatenate(pieces, axis=0).T.astype(jnp.bfloat16)
        tail_ref[...] = weight * tail

    above = jnp.dot(
        lhs_ref[pl.ds(0, width), :], above_ref[...], preferred_element_type=jnp.float32
    )
    right_ref[...] = weight * above[width - 1 : width, :]
    mirror = jnp.dot(
        lhs_ref[pl.ds(width, rounded_up(out_rows, 16)), :],
        mirror_ref[...],
        preferred_element_type=jnp.float32,
    )[:out_rows]
    mirror = (weight * mirror).astype(jnp.bfloat16)
    flip = (
        lax.broadcasted_iota(jnp.int32, (LANES, LANES), 0)
        + lax.broadcasted_iota(jnp.int32, (LANES, LANES), 1)
        == LANES - 1
    ).astype(jnp.float32).astype(jnp.bfloat16)
    flipped = jnp.concatenate(
        [
            jnp.dot(
                mirror[:, start : start + LANES], flip, preferred_element_type=jnp.float32
            )
            for start in range(tile_cols - LANES, -1, -LANES)
        ],
        axis=1,
    )
    cols = lax.broadcasted_iota(jnp.int32, (out_rows, tile_cols), 1) + tile * tile_cols
    fold_ref[...] = jnp.where(
        cols >= rows_ref[...], weight * above[:out_rows], flipped
    ).astype(fold_ref.dtype)


def on_device(
    design,
    nuisance_design,
    observed,
    arc_of_row,
    nuis_size,
    weight_index,
    kind_weight,
    mission_weight,
):
    groups = lax.axis_size("mission")
    members = lax.axis_size("arc")
    group = lax.axis_index("mission")
    member = lax.axis_index("arc")
    block_rows, width_all = design.shape
    half_width = width_all // 2
    final_rows = half_width // (groups * members)
    out_rows = groups * final_rows
    wide = rounded_up(block_rows + 1, LANES)
    width = rounded_up(out_rows + 1, LANES)
    vmem = pl.BlockSpec(memory_space=pltpu.VMEM)
    smem = pl.BlockSpec(memory_space=pltpu.SMEM)

    design_all = lax.all_gather(design, "arc", axis=0, tiled=True)

    proj = pl.pallas_call(
        projector_kernel,
        out_shape=jax.ShapeDtypeStruct((block_rows, wide), jnp.bfloat16),
        in_specs=[smem, smem, vmem, vmem, vmem, vmem, vmem],
        out_specs=vmem,
        cost_estimate=pl.CostEstimate(flops=10_000_000, bytes_accessed=100_000, transcendentals=0),
        name="projector",
    )(
        nuis_size,
        kind_weight,
        nuisance_design,
        arc_of_row[:, None],
        jnp.pad(arc_of_row, (0, wide - block_rows), constant_values=-1)[None, :],
        weight_index[:, None],
        jnp.pad(observed, (0, wide - block_rows))[None, :],
    )
    proj_all = lax.all_gather(proj, "arc", axis=0, tiled=True)

    def picked(start_of):
        parts = [
            lax.dynamic_slice_in_dim(
                design_all, start_of(other * members + member), final_rows, 1
            )
            for other in range(groups)
        ]
        blank = jnp.zeros((design_all.shape[0], width - out_rows), design_all.dtype)
        return parts + [blank]

    picked_all = jnp.concatenate(
        picked(lambda block: block * final_rows)
        + picked(lambda block: width_all - (block + 1) * final_rows)
        + picked(lambda block: half_width + block * final_rows),
        axis=1,
    )
    place = np.arange(out_rows)
    perm = np.zeros((width, width), np.float32)
    perm[(place // final_rows) * final_rows + final_rows - 1 - place % final_rows, place] = 1.0
    row_ids = (
        (jnp.arange(groups, dtype=jnp.int32)[:, None] * members + member) * final_rows
        + jnp.arange(final_rows, dtype=jnp.int32)[None, :]
    ).reshape(out_rows, 1)

    tile_cols = 512
    tiles = width_all // tile_cols
    all_rows = design_all.shape[0]
    whole = lambda shape: pl.BlockSpec(shape, lambda j: (0, 0))
    fold, right, tail = pl.pallas_call(
        functools.partial(fold_kernel, block_rows, width),
        grid=(tiles,),
        out_shape=(
            jax.ShapeDtypeStruct((out_rows, width_all), jnp.bfloat16),
            jax.ShapeDtypeStruct((1, width_all), jnp.float32),
            jax.ShapeDtypeStruct((1, width), jnp.float32),
        ),
        in_specs=[
            smem,
            whole((all_rows, wide)),
            whole((all_rows, 3 * width)),
            whole((width, width)),
            whole((out_rows, 1)),
            pl.BlockSpec((all_rows, tile_cols), lambda j: (0, j)),
            pl.BlockSpec((all_rows, tile_cols), lambda j: (0, tiles - 1 - j)),
        ],
        out_specs=(
            pl.BlockSpec((out_rows, tile_cols), lambda j: (0, j)),
            pl.BlockSpec((1, tile_cols), lambda j: (0, j)),
            whole((1, width)),
        ),
        scratch_shapes=[pltpu.VMEM((2 * width, all_rows), jnp.bfloat16)],
        compiler_params=pltpu.CompilerParams(
            dimension_semantics=("arbitrary",), vmem_limit_bytes=60 * 2**20
        ),
        cost_estimate=pl.CostEstimate(
            flops=4 * width * all_rows * width_all,
            bytes_accessed=4 * all_rows * width_all,
            transcendentals=0,
        ),
        name="fold",
    )(
        mission_weight,
        proj_all,
        picked_all,
        jnp.asarray(perm, jnp.bfloat16),
        row_ids,
        design_all,
        design_all,
    )

    right_own = lax.dynamic_index_in_dim(
        right.reshape(groups, members, width_all // (groups * members)), member, 1, keepdims=False
    )
    tail_own = tail[0, :out_rows].reshape(groups, final_rows)
    fold = fold.reshape(groups, final_rows, width_all)
    vectors = jnp.concatenate([right_own, tail_own], axis=1)

    def taken(array, index):
        return lax.dynamic_index_in_dim(array, index, 0, keepdims=False)

    fold_total = taken(fold, group).astype(jnp.float32)
    vector_total = taken(vectors, group)
    for shift in range(1, groups):
        ring = [(source, (source + shift) % groups) for source in range(groups)]
        target = (group + shift) % groups
        fold_total += lax.ppermute(taken(fold, target), "mission", ring).astype(jnp.float32)
        vector_total += lax.ppermute(taken(vectors, target), "mission", ring)
    split = right_own.shape[1]
    return (fold_total, vector_total[:split], vector_total[split:])


def solution(mesh):
    placed = (
        P(("mission", "arc"), None),
        P(("mission", "arc"), None),
        P(("mission", "arc")),
        P(("mission", "arc")),
        P(("mission", "arc")),
        P(("mission", "arc")),
        P(),
        P("mission"),
    )
    return jax.shard_map(
        on_device,
        mesh=mesh,
        in_specs=placed,
        out_specs=(P(("mission", "arc"), None), P(("mission", "arc")), P(("mission", "arc"))),
        check_vma=False,
    )
```

```python
import functools

import jax
import jax.numpy as jnp
import numpy as np
from jax import lax
from jax.experimental import pallas as pl
from jax.experimental.pallas import tpu as pltpu
from jax.sharding import PartitionSpec as P

LANES = 128


def rounded_up(value, unit):
    return -(-value // unit) * unit


def projector_kernel(
    sizes_ref, kinds_ref, nuis_ref, arc_col_ref, arc_row_ref, kind_col_ref, obs_row_ref, out_ref
):
    rows, wide = out_ref.shape
    arc_col = arc_col_ref[...]
    kind_col = kind_col_ref[...]
    weight = jnp.zeros((rows, 1), jnp.float32)
    for kind in range(kinds_ref.shape[0]):
        weight = jnp.where(kind_col == kind, kinds_ref[kind], weight)
    size = jnp.zeros((rows, 1), jnp.int32)
    for arc in range(sizes_ref.shape[0]):
        size = jnp.where(arc_col == arc, sizes_ref[arc], size)
    nuis = nuis_ref[...].astype(jnp.float32)
    nuis = jnp.where(lax.broadcasted_iota(jnp.int32, nuis.shape, 1) < size, nuis, 0.0)
    padded = jnp.concatenate(
        [nuis, jnp.zeros((wide - rows, nuis.shape[1]), jnp.float32)], axis=0
    )
    gram = lax.dot_general(
        nuis.astype(jnp.bfloat16),
        padded.astype(jnp.bfloat16),
        (((1,), (1,)), ((), ())),
        preferred_element_type=jnp.float32,
    )
    lane = lax.broadcasted_iota(jnp.int32, (rows, wide), 1)
    sub = lax.broadcasted_iota(jnp.int32, (rows, wide), 0)
    state = jnp.where(arc_col == arc_row_ref[...], gram, 0.0)
    state = state + jnp.where(lane == sub, 1.0 / weight, 0.0)
    for k in range(rows):
        row = state[k : k + 1, :]
        col = state[:, k : k + 1]
        inv = 1.0 / row[:, k : k + 1]
        scaled_row = row * inv
        scaled_col = col * inv
        swept = state - col * scaled_row
        swept = jnp.where(lane == k, scaled_col, swept)
        swept = jnp.where(sub == k, scaled_row, swept)
        state = jnp.where((lane == k) & (sub == k), -inv, swept)
    inverse = -state
    reduced_obs = jnp.sum(inverse * obs_row_ref[...], axis=1, keepdims=True)
    out_ref[...] = jnp.where(lane == rows, reduced_obs, inverse).astype(out_ref.dtype)


def fold_kernel(
    block_rows,
    width,
    with_right,
    weight_ref,
    span_ref,
    proj_ref,
    picked_ref,
    perm_ref,
    rows_ref,
    above_ref,
    mirror_ref,
    fold_ref,
    tail_ref,
    *rest,
):
    lhs_ref = rest[-1]
    tile = pl.program_id(0)
    tile_cols = above_ref.shape[1]
    out_rows = fold_ref.shape[0]
    weight = weight_ref[0]

    @pl.when(tile == 0)
    def _():
        tail = jnp.zeros((1, width), jnp.float32)
        lane = lax.broadcasted_iota(jnp.int32, (block_rows, width), 1)
        pieces = []
        for block in range(proj_ref.shape[0] // block_rows):
            span = pl.ds(block * block_rows, block_rows)
            proj = proj_ref[span, :]
            picked = picked_ref[span, :]
            reduced = lax.dot_general(
                proj[:, :block_rows], picked, (((1,), (0,)), ((), ())),
                preferred_element_type=jnp.float32,
            )
            tail_reduced = reduced[:, 2 * width :].astype(jnp.bfloat16).astype(jnp.float32)
            tail += jnp.sum(
                picked[:, 2 * width :].astype(jnp.float32) * tail_reduced, axis=0, keepdims=True
            )
            first = jnp.where(
                lane == width - 1,
                proj[:, block_rows : block_rows + 1].astype(jnp.float32),
                reduced[:, :width],
            )
            second = jnp.dot(
                reduced[:, width : 2 * width].astype(jnp.bfloat16),
                perm_ref[...],
                preferred_element_type=jnp.float32,
            )
            pieces.append(jnp.concatenate([first, second], axis=1))
        lhs_ref[...] = jnp.concatenate(pieces, axis=0).T.astype(jnp.bfloat16)
        tail_ref[...] = weight * tail

    low, high = span_ref[0], span_ref[1]
    col_start = tile * tile_cols
    all_above = col_start >= high
    all_mirror = col_start + tile_cols <= low

    def above_tile():
        return weight * jnp.dot(
            lhs_ref[pl.ds(0, width), :], above_ref[...], preferred_element_type=jnp.float32
        )

    def mirror_tile():
        mirror = jnp.dot(
            lhs_ref[pl.ds(width, rounded_up(out_rows, 16)), :],
            mirror_ref[...],
            preferred_element_type=jnp.float32,
        )[:out_rows]
        mirror = (weight * mirror).astype(jnp.bfloat16)
        flip = (
            lax.broadcasted_iota(jnp.int32, (LANES, LANES), 0)
            + lax.broadcasted_iota(jnp.int32, (LANES, LANES), 1)
            == LANES - 1
        ).astype(jnp.float32).astype(jnp.bfloat16)
        return jnp.concatenate(
            [
                jnp.dot(
                    mirror[:, start : start + LANES], flip, preferred_element_type=jnp.float32
                )
                for start in range(tile_cols - LANES, -1, -LANES)
            ],
            axis=1,
        )

    if with_right:
        above = above_tile()
        rest[0][...] = above[width - 1 : width, :]
        fold_ref[...] = above[:out_rows].astype(fold_ref.dtype)
    else:

        @pl.when(jnp.logical_not(all_mirror))
        def _():
            fold_ref[...] = above_tile()[:out_rows].astype(fold_ref.dtype)

    @pl.when(all_mirror)
    def _():
        fold_ref[...] = mirror_tile().astype(fold_ref.dtype)

    @pl.when(jnp.logical_not(jnp.logical_or(all_above, all_mirror)))
    def _():
        cols = lax.broadcasted_iota(jnp.int32, (out_rows, tile_cols), 1) + col_start
        fold_ref[...] = jnp.where(
            cols >= rows_ref[...], fold_ref[...].astype(jnp.float32), mirror_tile()
        ).astype(fold_ref.dtype)


def on_device(
    design,
    nuisance_design,
    observed,
    arc_of_row,
    nuis_size,
    weight_index,
    kind_weight,
    mission_weight,
):
    groups = lax.axis_size("mission")
    members = lax.axis_size("arc")
    group = lax.axis_index("mission")
    member = lax.axis_index("arc")
    block_rows, width_all = design.shape
    half_width = width_all // 2
    final_rows = half_width // (groups * members)
    wide = rounded_up(block_rows + 1, LANES)
    inner = 2 if members % 2 == 0 else 1
    outer = 4 if members % (4 * inner) == 0 else 1
    mid = members // (outer * inner)
    mid_at = (member // inner) % mid
    gather_groups = [
        [(o * mid + y) * inner + c for o in range(outer) for c in range(inner)]
        for y in range(mid)
    ]

    def gathered(array):
        return lax.all_gather(
            array, "arc", axis=0, tiled=True, axis_index_groups=gather_groups
        )

    def member_of(y):
        return (member // (inner * mid) * mid + y) * inner + member % inner

    vmem = pl.BlockSpec(memory_space=pltpu.VMEM)
    smem = pl.BlockSpec(memory_space=pltpu.SMEM)

    design_all = gathered(design)

    proj = pl.pallas_call(
        projector_kernel,
        out_shape=jax.ShapeDtypeStruct((block_rows, wide), jnp.bfloat16),
        in_specs=[smem, smem, vmem, vmem, vmem, vmem, vmem],
        out_specs=vmem,
        cost_estimate=pl.CostEstimate(flops=10_000_000, bytes_accessed=100_000, transcendentals=0),
        name="projector",
    )(
        nuis_size,
        kind_weight,
        nuisance_design,
        arc_of_row[:, None],
        jnp.pad(arc_of_row, (0, wide - block_rows), constant_values=-1)[None, :],
        weight_index[:, None],
        jnp.pad(observed, (0, wide - block_rows))[None, :],
    )
    proj_all = gathered(proj)

    shifts = [(dm, dy) for dm in range(groups) for dy in range(mid)]
    shifts.sort(key=lambda shift: -(shift[0] > 0) - (shift[1] > 0))
    per_call = max(1, len(shifts) // 4)
    out_rows = per_call * final_rows
    width = rounded_up(out_rows + 1, LANES)
    place = np.arange(out_rows)
    perm = np.zeros((width, width), np.float32)
    perm[(place // final_rows) * final_rows + final_rows - 1 - place % final_rows, place] = 1.0
    tile_cols = 512
    tiles = width_all // tile_cols
    all_rows = design_all.shape[0]
    right_cols = width_all // (groups * members)
    whole = lambda shape: pl.BlockSpec(shape, lambda j: (0, 0))

    def fold_call(owners, with_right):
        def picked(start_of):
            parts = [
                lax.dynamic_slice_in_dim(design_all, start_of(owner), final_rows, 1)
                for owner in owners
            ]
            blank = jnp.zeros((all_rows, width - out_rows), design_all.dtype)
            return parts + [blank]

        picked_all = jnp.concatenate(
            picked(lambda block: block * final_rows)
            + picked(lambda block: width_all - (block + 1) * final_rows)
            + picked(lambda block: half_width + block * final_rows),
            axis=1,
        )
        starts = jnp.stack(owners).astype(jnp.int32) * final_rows
        row_ids = (
            starts[:, None] + jnp.arange(final_rows, dtype=jnp.int32)[None, :]
        ).reshape(out_rows, 1)
        span = jnp.stack([jnp.min(starts), jnp.max(starts) + final_rows - 1])
        out_shape = [
            jax.ShapeDtypeStruct((out_rows, width_all), jnp.bfloat16),
            jax.ShapeDtypeStruct((1, width), jnp.float32),
        ]
        out_specs = [
            pl.BlockSpec((out_rows, tile_cols), lambda j: (0, j)),
            whole((1, width)),
        ]
        if with_right:
            out_shape.append(jax.ShapeDtypeStruct((1, width_all), jnp.float32))
            out_specs.append(pl.BlockSpec((1, tile_cols), lambda j: (0, j)))
        return pl.pallas_call(
            functools.partial(fold_kernel, block_rows, width, with_right),
            grid=(tiles,),
            out_shape=tuple(out_shape),
            in_specs=[
                smem,
                smem,
                whole((all_rows, wide)),
                whole((all_rows, 3 * width)),
                whole((width, width)),
                whole((out_rows, 1)),
                pl.BlockSpec((all_rows, tile_cols), lambda j: (0, j)),
                pl.BlockSpec((all_rows, tile_cols), lambda j: (0, tiles - 1 - j)),
            ],
            out_specs=tuple(out_specs),
            scratch_shapes=[pltpu.VMEM((2 * width, all_rows), jnp.bfloat16)],
            compiler_params=pltpu.CompilerParams(
                dimension_semantics=("arbitrary",), vmem_limit_bytes=60 * 2**20
            ),
            cost_estimate=pl.CostEstimate(
                flops=4 * width * all_rows * width_all,
                bytes_accessed=4 * all_rows * width_all,
                transcendentals=0,
            ),
            name="fold",
        )(
            mission_weight,
            span,
            proj_all,
            picked_all,
            jnp.asarray(perm, jnp.bfloat16),
            row_ids,
            design_all,
            design_all,
        )

    def ring(dm, dy):
        pairs = []
        for m in range(groups):
            for a in range(members):
                o, y, c = a // (inner * mid), (a // inner) % mid, a % inner
                target = (o * mid + (y + dy) % mid) * inner + c
                pairs.append((m * members + a, (m + dm) % groups * members + target))
        return pairs

    right = None
    folds, vectors = [], []
    for first in range(0, len(shifts), per_call):
        here = shifts[first : first + per_call]
        owners = [
            (group + dm) % groups * members + member_of((mid_at + dy) % mid) for dm, dy in here
        ]
        fold, tail, *extra = fold_call(owners, right is None)
        if right is None:
            right = extra[0][0]
        for at, (dm, dy) in enumerate(here):
            rows = slice(at * final_rows, (at + 1) * final_rows)
            block = fold[rows]
            vector = jnp.concatenate(
                [
                    lax.dynamic_slice_in_dim(right, owners[at] * right_cols, right_cols),
                    tail[0, rows],
                ]
            )
            if dm or dy:
                block = lax.ppermute(block, ("mission", "arc"), ring(dm, dy))
                vector = lax.ppermute(vector, ("mission", "arc"), ring(dm, dy))
            folds.append(block.astype(jnp.float32))
            vectors.append(vector)
    fold_total = functools.reduce(jnp.add, folds)
    vector_total = functools.reduce(jnp.add, vectors)
    return (fold_total, vector_total[:right_cols], vector_total[right_cols:])


def solution(mesh):
    placed = (
        P(("mission", "arc"), None),
        P(("mission", "arc"), None),
        P(("mission", "arc")),
        P(("mission", "arc")),
        P(("mission", "arc")),
        P(("mission", "arc")),
        P(),
        P("mission"),
    )
    return jax.shard_map(
        on_device,
        mesh=mesh,
        in_specs=placed,
        out_specs=(P(("mission", "arc"), None), P(("mission", "arc")), P(("mission", "arc"))),
        check_vma=False,
    )
```

```python
import functools

import jax
import jax.numpy as jnp
import numpy as np
from jax import lax
from jax.experimental import pallas as pl
from jax.experimental.pallas import tpu as pltpu
from jax.sharding import PartitionSpec as P

LANES = 128


def rounded_up(value, unit):
    return -(-value // unit) * unit


def projector_kernel(
    sizes_ref, kinds_ref, nuis_ref, arc_col_ref, arc_row_ref, kind_col_ref, obs_row_ref, out_ref
):
    rows, wide = out_ref.shape
    arc_col = arc_col_ref[...]
    kind_col = kind_col_ref[...]
    weight = jnp.zeros((rows, 1), jnp.float32)
    for kind in range(kinds_ref.shape[0]):
        weight = jnp.where(kind_col == kind, kinds_ref[kind], weight)
    size = jnp.zeros((rows, 1), jnp.int32)
    for arc in range(sizes_ref.shape[0]):
        size = jnp.where(arc_col == arc, sizes_ref[arc], size)
    nuis = nuis_ref[...].astype(jnp.float32)
    nuis = jnp.where(lax.broadcasted_iota(jnp.int32, nuis.shape, 1) < size, nuis, 0.0)
    padded = jnp.concatenate(
        [nuis, jnp.zeros((wide - rows, nuis.shape[1]), jnp.float32)], axis=0
    )
    gram = lax.dot_general(
        nuis.astype(jnp.bfloat16),
        padded.astype(jnp.bfloat16),
        (((1,), (1,)), ((), ())),
        preferred_element_type=jnp.float32,
    )
    lane = lax.broadcasted_iota(jnp.int32, (rows, wide), 1)
    sub = lax.broadcasted_iota(jnp.int32, (rows, wide), 0)
    state = jnp.where(arc_col == arc_row_ref[...], gram, 0.0)
    state = state + jnp.where(lane == sub, 1.0 / weight, 0.0)
    for k in range(rows):
        row = state[k : k + 1, :]
        col = state[:, k : k + 1]
        inv = 1.0 / row[:, k : k + 1]
        scaled_row = row * inv
        scaled_col = col * inv
        swept = state - col * scaled_row
        swept = jnp.where(lane == k, scaled_col, swept)
        swept = jnp.where(sub == k, scaled_row, swept)
        state = jnp.where((lane == k) & (sub == k), -inv, swept)
    inverse = -state
    reduced_obs = jnp.sum(inverse * obs_row_ref[...], axis=1, keepdims=True)
    out_ref[...] = jnp.where(lane == rows, reduced_obs, inverse).astype(out_ref.dtype)


def fold_kernel(
    block_rows,
    width,
    with_right,
    weight_ref,
    span_ref,
    proj_ref,
    picked_ref,
    perm_ref,
    rows_ref,
    above_ref,
    mirror_ref,
    fold_ref,
    tail_ref,
    *rest,
):
    lhs_ref = rest[-1]
    tile = pl.program_id(0)
    tile_cols = above_ref.shape[1]
    out_rows = fold_ref.shape[0]
    weight = weight_ref[0]

    @pl.when(tile == 0)
    def _():
        tail = jnp.zeros((1, width), jnp.float32)
        lane = lax.broadcasted_iota(jnp.int32, (block_rows, width), 1)
        pieces = []
        for block in range(proj_ref.shape[0] // block_rows):
            span = pl.ds(block * block_rows, block_rows)
            proj = proj_ref[span, :]
            picked = picked_ref[span, :]
            reduced = lax.dot_general(
                proj[:, :block_rows], picked, (((1,), (0,)), ((), ())),
                preferred_element_type=jnp.float32,
            )
            tail_reduced = reduced[:, 2 * width :].astype(jnp.bfloat16).astype(jnp.float32)
            tail += jnp.sum(
                picked[:, 2 * width :].astype(jnp.float32) * tail_reduced, axis=0, keepdims=True
            )
            first = jnp.where(
                lane == width - 1,
                proj[:, block_rows : block_rows + 1].astype(jnp.float32),
                reduced[:, :width],
            )
            second = jnp.dot(
                reduced[:, width : 2 * width].astype(jnp.bfloat16),
                perm_ref[...],
                preferred_element_type=jnp.float32,
            )
            pieces.append(jnp.concatenate([first, second], axis=1))
        lhs_ref[...] = jnp.concatenate(pieces, axis=0).T.astype(jnp.bfloat16)
        tail_ref[...] = weight * tail

    low, high = span_ref[0], span_ref[1]
    col_start = tile * tile_cols
    all_above = col_start >= high
    all_mirror = col_start + tile_cols <= low

    def above_tile():
        return weight * jnp.dot(
            lhs_ref[pl.ds(0, width), :], above_ref[...], preferred_element_type=jnp.float32
        )

    def mirror_tile():
        mirror = jnp.dot(
            lhs_ref[pl.ds(width, rounded_up(out_rows, 16)), :],
            mirror_ref[...],
            preferred_element_type=jnp.float32,
        )[:out_rows]
        mirror = (weight * mirror).astype(jnp.bfloat16)
        flip = (
            lax.broadcasted_iota(jnp.int32, (LANES, LANES), 0)
            + lax.broadcasted_iota(jnp.int32, (LANES, LANES), 1)
            == LANES - 1
        ).astype(jnp.float32).astype(jnp.bfloat16)
        return jnp.concatenate(
            [
                jnp.dot(
                    mirror[:, start : start + LANES], flip, preferred_element_type=jnp.float32
                )
                for start in range(tile_cols - LANES, -1, -LANES)
            ],
            axis=1,
        )

    if with_right:
        above = above_tile()
        rest[0][...] = above[width - 1 : width, :]
        fold_ref[...] = above[:out_rows].astype(fold_ref.dtype)
    else:

        @pl.when(jnp.logical_not(all_mirror))
        def _():
            fold_ref[...] = above_tile()[:out_rows].astype(fold_ref.dtype)

    @pl.when(all_mirror)
    def _():
        fold_ref[...] = mirror_tile().astype(fold_ref.dtype)

    @pl.when(jnp.logical_not(jnp.logical_or(all_above, all_mirror)))
    def _():
        cols = lax.broadcasted_iota(jnp.int32, (out_rows, tile_cols), 1) + col_start
        fold_ref[...] = jnp.where(
            cols >= rows_ref[...], fold_ref[...].astype(jnp.float32), mirror_tile()
        ).astype(fold_ref.dtype)


def on_device(
    design,
    nuisance_design,
    observed,
    arc_of_row,
    nuis_size,
    weight_index,
    kind_weight,
    mission_weight,
):
    groups = lax.axis_size("mission")
    members = lax.axis_size("arc")
    group = lax.axis_index("mission")
    member = lax.axis_index("arc")
    block_rows, width_all = design.shape
    half_width = width_all // 2
    final_rows = half_width // (groups * members)
    wide = rounded_up(block_rows + 1, LANES)
    inner = 2 if members % 2 == 0 else 1
    outer = 4 if members % (4 * inner) == 0 else 1
    mid = members // (outer * inner)
    mid_at = (member // inner) % mid
    gather_groups = [
        [(o * mid + y) * inner + c for o in range(outer) for c in range(inner)]
        for y in range(mid)
    ]

    def gathered(array):
        return lax.all_gather(
            array, "arc", axis=0, tiled=True, axis_index_groups=gather_groups
        )

    def member_of(y):
        return (member // (inner * mid) * mid + y) * inner + member % inner

    vmem = pl.BlockSpec(memory_space=pltpu.VMEM)
    smem = pl.BlockSpec(memory_space=pltpu.SMEM)

    design_all = gathered(design)

    proj = pl.pallas_call(
        projector_kernel,
        out_shape=jax.ShapeDtypeStruct((block_rows, wide), jnp.bfloat16),
        in_specs=[smem, smem, vmem, vmem, vmem, vmem, vmem],
        out_specs=vmem,
        cost_estimate=pl.CostEstimate(flops=10_000_000, bytes_accessed=100_000, transcendentals=0),
        name="projector",
    )(
        nuis_size,
        kind_weight,
        nuisance_design,
        arc_of_row[:, None],
        jnp.pad(arc_of_row, (0, wide - block_rows), constant_values=-1)[None, :],
        weight_index[:, None],
        jnp.pad(observed, (0, wide - block_rows))[None, :],
    )
    proj_all = gathered(proj)

    shifts = [(dm, dy) for dm in range(groups) for dy in range(mid)]
    shifts.sort(key=lambda shift: (shift[0] == 0, shift[1] == 0))
    per_call = max(1, len(shifts) // 2)
    out_rows = per_call * final_rows
    width = rounded_up(out_rows + 1, LANES)
    place = np.arange(out_rows)
    perm = np.zeros((width, width), np.float32)
    perm[(place // final_rows) * final_rows + final_rows - 1 - place % final_rows, place] = 1.0
    tile_cols = 512
    tiles = width_all // tile_cols
    all_rows = design_all.shape[0]
    right_cols = width_all // (groups * members)
    whole = lambda shape: pl.BlockSpec(shape, lambda j: (0, 0))

    def fold_call(owners, with_right):
        def picked(start_of):
            parts = [
                lax.dynamic_slice_in_dim(design_all, start_of(owner), final_rows, 1)
                for owner in owners
            ]
            blank = jnp.zeros((all_rows, width - out_rows), design_all.dtype)
            return parts + [blank]

        picked_all = jnp.concatenate(
            picked(lambda block: block * final_rows)
            + picked(lambda block: width_all - (block + 1) * final_rows)
            + picked(lambda block: half_width + block * final_rows),
            axis=1,
        )
        starts = jnp.stack(owners).astype(jnp.int32) * final_rows
        row_ids = (
            starts[:, None] + jnp.arange(final_rows, dtype=jnp.int32)[None, :]
        ).reshape(out_rows, 1)
        span = jnp.stack([jnp.min(starts), jnp.max(starts) + final_rows - 1])
        out_shape = [
            jax.ShapeDtypeStruct((out_rows, width_all), jnp.bfloat16),
            jax.ShapeDtypeStruct((1, width), jnp.float32),
        ]
        out_specs = [
            pl.BlockSpec((out_rows, tile_cols), lambda j: (0, j)),
            whole((1, width)),
        ]
        if with_right:
            out_shape.append(jax.ShapeDtypeStruct((1, width_all), jnp.float32))
            out_specs.append(pl.BlockSpec((1, tile_cols), lambda j: (0, j)))
        return pl.pallas_call(
            functools.partial(fold_kernel, block_rows, width, with_right),
            grid=(tiles,),
            out_shape=tuple(out_shape),
            in_specs=[
                smem,
                smem,
                whole((all_rows, wide)),
                whole((all_rows, 3 * width)),
                whole((width, width)),
                whole((out_rows, 1)),
                pl.BlockSpec((all_rows, tile_cols), lambda j: (0, j)),
                pl.BlockSpec((all_rows, tile_cols), lambda j: (0, tiles - 1 - j)),
            ],
            out_specs=tuple(out_specs),
            scratch_shapes=[pltpu.VMEM((2 * width, all_rows), jnp.bfloat16)],
            compiler_params=pltpu.CompilerParams(
                dimension_semantics=("arbitrary",), vmem_limit_bytes=60 * 2**20
            ),
            cost_estimate=pl.CostEstimate(
                flops=4 * width * all_rows * width_all,
                bytes_accessed=4 * all_rows * width_all,
                transcendentals=0,
            ),
            name="fold",
        )(
            mission_weight,
            span,
            proj_all,
            picked_all,
            jnp.asarray(perm, jnp.bfloat16),
            row_ids,
            design_all,
            design_all,
        )

    def ring(dm, dy):
        pairs = []
        for m in range(groups):
            for a in range(members):
                o, y, c = a // (inner * mid), (a // inner) % mid, a % inner
                target = (o * mid + (y + dy) % mid) * inner + c
                pairs.append((m * members + a, (m + dm) % groups * members + target))
        return pairs

    right = None
    folds, vectors = [], []
    for first in range(0, len(shifts), per_call):
        here = shifts[first : first + per_call]
        owners = [
            (group + dm) % groups * members + member_of((mid_at + dy) % mid) for dm, dy in here
        ]
        fold, tail, *extra = fold_call(owners, right is None)
        if right is None:
            right = extra[0][0]
        for at, (dm, dy) in enumerate(here):
            rows = slice(at * final_rows, (at + 1) * final_rows)
            block = fold[rows]
            vector = jnp.concatenate(
                [
                    lax.dynamic_slice_in_dim(right, owners[at] * right_cols, right_cols),
                    tail[0, rows],
                ]
            )
            if dm or dy:
                block = lax.ppermute(block, ("mission", "arc"), ring(dm, dy))
                vector = lax.ppermute(vector, ("mission", "arc"), ring(dm, dy))
            folds.append(block.astype(jnp.float32))
            vectors.append(vector)
    fold_total = functools.reduce(jnp.add, folds)
    vector_total = functools.reduce(jnp.add, vectors)
    return (fold_total, vector_total[:right_cols], vector_total[right_cols:])


def solution(mesh):
    placed = (
        P(("mission", "arc"), None),
        P(("mission", "arc"), None),
        P(("mission", "arc")),
        P(("mission", "arc")),
        P(("mission", "arc")),
        P(("mission", "arc")),
        P(),
        P("mission"),
    )
    return jax.shard_map(
        on_device,
        mesh=mesh,
        in_specs=placed,
        out_specs=(P(("mission", "arc"), None), P(("mission", "arc")), P(("mission", "arc"))),
        check_vma=False,
    )
```
